8 devices in a mesh: dp: 1 (over z), ty: 2 (over y), tx: 4 (over x, core).
Axes of the slice: x: 2, y: 2, z: 1, core: 2. Of those that a mesh axis runs over, the one named last changes fastest.
Arguments:
- hidden: bfloat16 [8192, 2048], P(('dp', 'ty'), 'tx')
- positions: int32 [8192], P(('dp', 'tx'))
- g_ffn: bfloat16 [2048], P('tx')
- w_gate: bfloat16 [2048, 5632], P('tx', 'ty')
- w_up: bfloat16 [2048, 5632], P('tx', 'ty')
- w_down: bfloat16 [5632, 2048], P('ty', 'tx')
- g_attn: bfloat16 [2048], P('tx')
- w_q: bfloat16 [2048, 32, 64], P('tx', 'ty')
- w_kv: bfloat16 [2048, 8, 64], P('tx', 'ty')
- grad_h2: bfloat16 [8192, 2048], P(('dp', 'ty'), 'tx')
- grad_q: bfloat16 [8192, 32, 64], P(('dp', 'tx'), 'ty')
- grad_kv: bfloat16 [8192, 8, 64], P(('dp', 'tx'), 'ty')
Outputs:
- output 1: bfloat16 [8192, 2048], P(('dp', 'ty'), 'tx')
- output 2: bfloat16 [8192, 32, 64], P(('dp', 'tx'), 'ty')
- output 3: bfloat16 [8192, 8, 64], P(('dp', 'tx'), 'ty')
- output 4: bfloat16 [8192, 2048], P(('dp', 'ty'), 'tx')
- output 5: float32 [2048], P(('dp', 'tx'))
- output 6: float32 [2048], P(('dp', 'tx'))
- output 7: float32 [2048, 5632], P(('dp', 'tx'), 'ty')
- output 8: float32 [2048, 5632], P(('dp', 'tx'), 'ty')
- output 9: float32 [5632, 2048], P(('dp', 'ty'), 'tx')
- output 10: float32 [2048, 32, 64], P(('dp', 'tx'), 'ty')
- output 11: float32 [2048, 8, 64], P(('dp', 'tx'), 'ty')
All inputs are finite; a program needn't handle non-finite values.
Results may differ from the reference program's by a relative error of at most 0.0196455.
Values are sent between devices in bfloat16 or wider.
A program may use at most 1 GiB of HBM per device.

```python
import jax
import jax.numpy as jnp
from jax import lax

TOKENS = 8192
MODEL_DIM = 2048
FFN_DIM = 5632
NUM_HEADS = 32
KV_HEADS = 4
HEAD_DIM = 64
MAX_POS = 4096
KV_SLOTS = 2 * KV_HEADS
NORM_EPS = 1e-5
ROPE_BASE = 10000.0


def setup_inputs(seed: int = 0, part: int = 0) -> dict:
    part_keys = jax.random.split(jax.random.fold_in(jax.random.key(seed), part), 7)
    shared_keys = jax.random.split(jax.random.key(seed + 7919), 7)
    row_tilt = jax.random.uniform(part_keys[0], (TOKENS, 1), minval=-0.8, maxval=0.8)
    row_level = jax.random.uniform(part_keys[1], (TOKENS, 1), minval=-0.5, maxval=0.5)
    col_wave = jnp.cos(jnp.pi * (jnp.arange(MODEL_DIM, dtype=jnp.float32) + 0.5) / MODEL_DIM)
    hidden = jax.random.normal(part_keys[2], (TOKENS, MODEL_DIM)) * jnp.exp(row_tilt * col_wave[None, :] + row_level)
    positions = jax.random.randint(part_keys[3], (TOKENS,), 0, MAX_POS, dtype=jnp.int32)
    grad_h2 = jax.random.normal(part_keys[4], (TOKENS, MODEL_DIM))
    grad_q = jax.random.normal(part_keys[5], (TOKENS, NUM_HEADS, HEAD_DIM))
    grad_kv = jax.random.normal(part_keys[6], (TOKENS, KV_SLOTS, HEAD_DIM))
    g_ffn = 1.0 + 0.3 * jax.random.normal(shared_keys[0], (MODEL_DIM,))
    g_attn = 1.0 + 0.3 * jax.random.normal(shared_keys[1], (MODEL_DIM,))
    w_gate = jax.random.normal(shared_keys[2], (MODEL_DIM, FFN_DIM)) * MODEL_DIM ** -0.5
    w_up = jax.random.normal(shared_keys[3], (MODEL_DIM, FFN_DIM)) * MODEL_DIM ** -0.5
    w_down = jax.random.normal(shared_keys[4], (FFN_DIM, MODEL_DIM)) * FFN_DIM ** -0.5
    w_q = jax.random.normal(shared_keys[5], (MODEL_DIM, NUM_HEADS, HEAD_DIM)) * MODEL_DIM ** -0.5
    w_kv = jax.random.normal(shared_keys[6], (MODEL_DIM, KV_SLOTS, HEAD_DIM)) * MODEL_DIM ** -0.5
    return {
        "hidden": hidden.astype(jnp.bfloat16),
        "positions": positions,
        "g_ffn": g_ffn.astype(jnp.bfloat16),
        "w_gate": w_gate.astype(jnp.bfloat16),
        "w_up": w_up.astype(jnp.bfloat16),
        "w_down": w_down.astype(jnp.bfloat16),
        "g_attn": g_attn.astype(jnp.bfloat16),
        "w_q": w_q.astype(jnp.bfloat16),
        "w_kv": w_kv.astype(jnp.bfloat16),
        "grad_h2": grad_h2.astype(jnp.bfloat16),
        "grad_q": grad_q.astype(jnp.bfloat16),
        "grad_kv": grad_kv.astype(jnp.bfloat16),
    }


def rms_scale(values):
    return lax.rsqrt(jnp.mean(values * values, axis=-1, keepdims=True) + NORM_EPS)


def rms_backward(values, inv_rms, gain, grad_out):
    scaled = grad_out * gain.astype(jnp.float32)
    grad_gain = jnp.sum(grad_out * values * inv_rms, axis=0)
    inner_dot = jnp.mean(scaled * values, axis=-1, keepdims=True)
    grad_in = inv_rms * scaled - values * (inv_rms * inv_rms * inv_rms) * inner_dot
    return grad_gain, grad_in


def rope_tables(positions):
    inv_freq = ROPE_BASE ** (-jnp.arange(0, HEAD_DIM, 2, dtype=jnp.float32) / HEAD_DIM)
    angles = positions.astype(jnp.float32)[:, None] * inv_freq[None, :]
    return jnp.cos(angles)[:, None, :], jnp.sin(angles)[:, None, :]


def rotate(values, cos_h, sin_h):
    pair_view = values.reshape(values.shape[:-1] + (values.shape[-1] // 2, 2))
    even_part = pair_view[..., 0]
    odd_part = pair_view[..., 1]
    turned = jnp.stack([even_part * cos_h - odd_part * sin_h, even_part * sin_h + odd_part * cos_h], axis=-1)
    return turned.reshape(values.shape)


def reference(hidden, positions, g_ffn, w_gate, w_up, w_down, g_attn, w_q, w_kv, grad_h2, grad_q, grad_kv):
    hidden_wide = hidden.astype(jnp.float32)
    inv_ffn = rms_scale(hidden_wide)
    normed = (hidden_wide * inv_ffn * g_ffn.astype(jnp.float32)).astype(jnp.bfloat16)
    gate_pre = jnp.dot(normed, w_gate, preferred_element_type=jnp.float32).astype(jnp.bfloat16).astype(jnp.float32)
    up_pre = jnp.dot(normed, w_up, preferred_element_type=jnp.float32).astype(jnp.bfloat16).astype(jnp.float32)
    gate_sig = jax.nn.sigmoid(gate_pre)
    hidden_act = (gate_pre * gate_sig * up_pre).astype(jnp.bfloat16)
    mlp_out = jnp.dot(hidden_act, w_down, preferred_element_type=jnp.float32)
    resid = (hidden_wide + mlp_out).astype(jnp.bfloat16)
    resid_wide = resid.astype(jnp.float32)
    inv_attn = rms_scale(resid_wide)
    normed2 = (resid_wide * inv_attn * g_attn.astype(jnp.float32)).astype(jnp.bfloat16)
    cos_t, sin_t = rope_tables(positions)
    kv_flag = (jnp.arange(KV_SLOTS) < KV_HEADS).astype(jnp.float32)[None, :, None]
    cos_kv = kv_flag * cos_t + (1.0 - kv_flag)
    sin_kv = kv_flag * sin_t
    normed2_wide = normed2.astype(jnp.float32)
    q_proj = jnp.einsum("td,dhk->thk", normed2_wide, w_q.astype(jnp.float32))
    kv_proj = jnp.einsum("td,dhk->thk", normed2_wide, w_kv.astype(jnp.float32))
    q_out = rotate(q_proj, cos_t, sin_t).astype(jnp.bfloat16)
    kv_out = rotate(kv_proj, cos_kv, sin_kv).astype(jnp.bfloat16)
    back_q = rotate(grad_q.astype(jnp.float32), cos_t, -sin_t).astype(jnp.bfloat16).astype(jnp.float32)
    back_kv = rotate(grad_kv.astype(jnp.float32), cos_kv, -sin_kv).astype(jnp.bfloat16).astype(jnp.float32)
    grad_wq = jnp.einsum("td,thk->dhk", normed2_wide, back_q)
    grad_wkv = jnp.einsum("td,thk->dhk", normed2_wide, back_kv)
    grad_n2 = jnp.einsum("thk,dhk->td", back_q, w_q.astype(jnp.float32)) + jnp.einsum("thk,dhk->td", back_kv, w_kv.astype(jnp.float32))
    grad_gattn, grad_attn_in = rms_backward(resid_wide, inv_attn, g_attn, grad_n2)
    grad_res = grad_h2.astype(jnp.float32) + grad_attn_in
    res_half = grad_res.astype(jnp.bfloat16)
    grad_wdown = jnp.dot(hidden_act.T, res_half, preferred_element_type=jnp.float32)
    grad_act = jnp.dot(res_half, w_down.T, preferred_element_type=jnp.float32)
    grad_gate = (grad_act * up_pre * gate_sig * (1.0 + gate_pre * (1.0 - gate_sig))).astype(jnp.bfloat16)
    grad_up = (grad_act * gate_pre * gate_sig).astype(jnp.bfloat16)
    grad_wgate = jnp.dot(normed.T, grad_gate, preferred_element_type=jnp.float32)
    grad_wup = jnp.dot(normed.T, grad_up, preferred_element_type=jnp.float32)
    grad_n = jnp.dot(grad_gate, w_gate.T, preferred_element_type=jnp.float32) + jnp.dot(grad_up, w_up.T, preferred_element_type=jnp.float32)
    grad_gffn, grad_ffn_in = rms_backward(hidden_wide, inv_ffn, g_ffn, grad_n)
    grad_hidden = (grad_res + grad_ffn_in).astype(jnp.bfloat16)
    return (resid, q_out, kv_out, grad_hidden, grad_gffn, grad_gattn, grad_wgate, grad_wup, grad_wdown, grad_wq, grad_wkv)
```

```python
import jax
import jax.numpy as jnp
from jax import lax
from jax.sharding import PartitionSpec as P

NORM_EPS = 1e-5
ROPE_BASE = 10000.0
F32 = jnp.float32
BF16 = jnp.bfloat16
AXES = ("ty", "tx")
ROWS = (((0,), (0,)), ((), ()))
COLS = (((1,), (1,)), ((), ()))


def dev(y, x, c):
    return y * 4 + x * 2 + c


ALL = [(y, x, c) for y in (0, 1) for x in (0, 1) for c in (0, 1)]
PERM_X = [(dev(y, x, c), dev(y, 1 - x, c)) for y, x, c in ALL]
PERM_Y = [(dev(y, x, c), dev(1 - y, x, c)) for y, x, c in ALL]
PERM_C = [(dev(y, x, c), dev(y, x, 1 - c)) for y, x, c in ALL]
HOME = [(x, x, c) for x in (0, 1) for c in (0, 1)]
AWAY = [(1 - x, x, c) for x in (0, 1) for c in (0, 1)]
IN_A = [(dev(y, x, c), dev(1 - y, x, c)) for y, x, c in HOME] + [(dev(y, x, c), dev(y, 1 - x, c)) for y, x, c in AWAY]
IN_B = [(dev(y, x, c), dev(1 - y, x, 1 - c)) for y, x, c in HOME] + [(dev(y, x, c), dev(y, 1 - x, 1 - c)) for y, x, c in AWAY]
IN_C1 = [(dev(y, x, c), dev(y, x, 1 - c)) for y, x, c in HOME]
IN_Y = [(dev(y, x, c), dev(1 - y, x, c)) for y, x, c in AWAY]
IN_CX = [(dev(y, x, c), dev(y, 1 - x, c)) for y, x, c in HOME]
IN_DX = [(dev(y, x, c), dev(y, 1 - x, 1 - c)) for y, x, c in HOME]


def inverse(perm):
    return [(b, a) for a, b in perm]


def send(value, perm):
    return lax.ppermute(value, AXES, perm)


def dot(a, b, dims=(((1,), (0,)), ((), ()))):
    return lax.dot_general(a, b, dims, preferred_element_type=F32)


def rotate(values, cos_h, sin_h):
    pair_view = values.reshape(values.shape[:-1] + (values.shape[-1] // 2, 2))
    even_part = pair_view[..., 0]
    odd_part = pair_view[..., 1]
    turned = jnp.stack([even_part * cos_h - odd_part * sin_h, even_part * sin_h + odd_part * cos_h], axis=-1)
    return turned.reshape(values.shape)


def rope_tables(positions, head_dim):
    inv_freq = ROPE_BASE ** (-jnp.arange(0, head_dim, 2, dtype=F32) / head_dim)
    angles = positions.astype(F32)[:, None] * inv_freq[None, :]
    return jnp.cos(angles)[:, None, :], jnp.sin(angles)[:, None, :]


def inv_rms(wide):
    return lax.rsqrt(jnp.mean(wide * wide, axis=1, keepdims=True) + NORM_EPS)


def norm_backward(values, inv, gain, grad_out):
    scaled = grad_out * gain
    grad_gain = jnp.sum(grad_out * values * inv, axis=0)
    inner = jnp.mean(scaled * values, axis=1, keepdims=True)
    return grad_gain, inv * scaled - values * (inv * inv * inv) * inner


def solution(mesh):
    ty_size = mesh.shape["ty"]

    def local_step(hidden, positions, g_ffn, w_gate, w_up, w_down, g_attn, w_q, w_kv, grad_h2, grad_q, grad_kv):
        y = lax.axis_index("ty")
        tx = lax.axis_index("tx")
        x = tx // 2
        c = tx % 2
        home = x == y
        half = jnp.where(home, 0, 1)
        rows = hidden.shape[0] // 4
        width = hidden.shape[1]
        tokens = 2 * rows
        head_dim = w_q.shape[2]
        kv_local = w_kv.shape[1]
        heads = w_q.shape[1]

        def gather_w(shard, axis):
            s1 = send(shard, PERM_X)
            s2 = send(shard, PERM_C)
            s3 = send(s1, PERM_C)
            return jnp.concatenate([shard, s1, s2, s3], axis=axis)

        def bring(array):
            view = array.reshape(2, 2, rows, width)
            same = lax.dynamic_index_in_dim(view, c, 0, keepdims=False)
            other = lax.dynamic_index_in_dim(view, 1 - c, 0, keepdims=False)
            same_h = lax.dynamic_index_in_dim(same, 1 - half, 0, keepdims=False)
            other_h = lax.dynamic_index_in_dim(other, 1 - half, 0, keepdims=False)
            pa = send(same_h, IN_A)
            pb = send(other_h, IN_B)
            pc = send(other[0], IN_C1)
            dy = send(jnp.stack([same[1], other[1]]), IN_Y)
            pcx = send(dy[0], IN_CX)
            pdx = send(dy[1], IN_DX)
            s0 = jnp.where(home, same[0], pa)
            s1 = jnp.where(home, pa, pcx)
            s2 = jnp.where(home, pc, pb)
            s3 = jnp.where(home, pb, pdx)
            return jnp.concatenate([s0, s1, s2, s3], axis=1)

        def give(block):
            s0, s1, s2, s3 = (block[:, k * width:(k + 1) * width] for k in range(4))
            pa = send(jnp.where(home, s1, s0), inverse(IN_A))
            pb = send(jnp.where(home, s3, s2), inverse(IN_B))
            pc = send(s2, IN_C1)
            pcx = send(s1, inverse(IN_CX))
            pdx = send(s3, inverse(IN_DX))
            dy = send(jnp.stack([pcx, pdx]), inverse(IN_Y))
            same = jnp.where(home, jnp.stack([s0, pa]), jnp.stack([pa, dy[0]]))
            other = jnp.where(home, jnp.stack([pc, pb]), jnp.stack([pb, dy[1]]))
            first = jnp.where(c == 0, same, other)
            second = jnp.where(c == 0, other, same)
            return jnp.concatenate([first, second], axis=0).reshape(4 * rows, width)

        def scatter_w(low, high, axis, shape=None):
            got = send(high.astype(BF16), PERM_C)
            total = low + got.astype(F32)
            n = total.shape[axis] // 2
            mine = lax.slice_in_dim(total, 0, n, axis=axis)
            theirs = lax.slice_in_dim(total, n, 2 * n, axis=axis)
            got = send(theirs.astype(BF16), PERM_X)
            return mine + got.astype(F32)

        def mine_other(array):
            view = array.reshape((2, rows) + array.shape[1:])
            return (lax.dynamic_index_in_dim(view, half, 0, keepdims=False),
                    lax.dynamic_index_in_dim(view, 1 - half, 0, keepdims=False))

        def canonical(mine, other):
            return jnp.where(home, jnp.concatenate([mine, other], axis=0), jnp.concatenate([other, mine], axis=0))

        def reduce_gain(vec):
            vec = vec + send(vec, PERM_Y)
            n = vec.shape[0] // 2
            vec = vec[:n] + send(vec[n:], PERM_C)
            return vec[:n // 2] + send(vec[n // 2:], PERM_X)

        wq = gather_w(w_q.reshape(width, heads * head_dim), 0)
        wkv = gather_w(w_kv.reshape(width, kv_local * head_dim), 0)
        h_m = bring(hidden)
        h_o = send(h_m, PERM_Y)
        wg = gather_w(w_gate, 0)
        wu = gather_w(w_up, 0)
        wd = gather_w(w_down, 1)
        gh_m = bring(grad_h2)
        gains = jnp.stack([g_ffn, g_attn]).astype(F32)
        gains = gather_w(gains, 1)
        gain_ffn, gain_attn = gains[0], gains[1]

        cos_t, sin_t = rope_tables(positions, head_dim)
        kv_index = y * kv_local + jnp.arange(kv_local)
        kv_flag = (kv_index < kv_local * ty_size // 2).astype(F32)[None, :, None]
        cos_kv = kv_flag * cos_t + (1.0 - kv_flag)
        sin_kv = kv_flag * sin_t
        back_q = rotate(grad_q.astype(F32), cos_t, -sin_t).astype(BF16).reshape(tokens, heads * head_dim)
        back_kv = rotate(grad_kv.astype(F32), cos_kv, -sin_kv).astype(BF16).reshape(tokens, kv_local * head_dim)
        eq_m, eq_o = mine_other(back_q)
        ekv_m, ekv_o = mine_other(back_kv)

        dn2_o = (dot(eq_o, wq, COLS) + dot(ekv_o, wkv, COLS)).astype(BF16)
        dn2_got = send(dn2_o, PERM_Y)
        dn2_m = dot(eq_m, wq, COLS) + dot(ekv_m, wkv, COLS) + dn2_got.astype(F32)

        hw_m = h_m.astype(F32)
        r1_m = inv_rms(hw_m)
        n_m = (hw_m * r1_m * gain_ffn).astype(BF16)
        hw_o = h_o.astype(F32)
        n_o = (hw_o * inv_rms(hw_o) * gain_ffn).astype(BF16)

        def gated(n):
            a = dot(n, wg).astype(BF16)
            b = dot(n, wu).astype(BF16)
            aw = a.astype(F32)
            u = (aw * jax.nn.sigmoid(aw) * b.astype(F32)).astype(BF16)
            return a, b, u

        a_o, b_o, u_o = gated(n_o)
        a_m, b_m, u_m = gated(n_m)
        mlp_got = send(dot(u_o, wd).astype(BF16), PERM_Y)
        mlp_m = dot(u_m, wd) + mlp_got.astype(F32)
        h2_m = (hw_m + mlp_m).astype(BF16)
        h2w_m = h2_m.astype(F32)
        r2_m = inv_rms(h2w_m)
        n2_m = (h2w_m * r2_m * gain_attn).astype(BF16)

        gg_attn, dx2 = norm_backward(h2w_m, r2_m, gain_attn, dn2_m)
        dres_m = gh_m.astype(F32) + dx2
        e_m = dres_m.astype(BF16)
        e_o = send(e_m, PERM_Y)
        n2_o = send(n2_m, PERM_Y)

        def act_back(e, a, b):
            du = dot(e, wd, COLS)
            aw = a.astype(F32)
            s = jax.nn.sigmoid(aw)
            da = (du * b.astype(F32) * s * (1.0 + aw * (1.0 - s))).astype(BF16)
            db = (du * aw * s).astype(BF16)
            return da, db

        da_m, db_m = act_back(e_m, a_m, b_m)
        da_o, db_o = act_back(e_o, a_o, b_o)
        dn_got = send((dot(da_o, wg, COLS) + dot(db_o, wu, COLS)).astype(BF16), PERM_Y)
        dn_m = dot(da_m, wg, COLS) + dot(db_m, wu, COLS) + dn_got.astype(F32)
        gg_ffn, dx1 = norm_backward(hw_m, r1_m, gain_ffn, dn_m)
        dh_m = (dres_m + dx1).astype(BF16)

        cat = lambda m, o: jnp.concatenate([m, o], axis=0)
        n_all, da, db, u, e, n2 = cat(n_m, n_o), cat(da_m, da_o), cat(db_m, db_o), cat(u_m, u_o), cat(e_m, e_o), cat(n2_m, n2_o)
        eq, ekv = cat(eq_m, eq_o), cat(ekv_m, ekv_o)
        k = 2 * width
        gw_down = scatter_w(dot(u, e[:, :k], ROWS), dot(u, e[:, k:], ROWS), 1)
        gw_gate = scatter_w(dot(n_all[:, :k], da, ROWS), dot(n_all[:, k:], da, ROWS), 0)
        gw_up = scatter_w(dot(n_all[:, :k], db, ROWS), dot(n_all[:, k:], db, ROWS), 0)
        gw_q = scatter_w(dot(n2[:, :k], eq, ROWS), dot(n2[:, k:], eq, ROWS), 0)
        gw_kv = scatter_w(dot(n2[:, :k], ekv, ROWS), dot(n2[:, k:], ekv, ROWS), 0)

        def proj(n2h, w):
            return dot(n2h, w)
        q = canonical(proj(n2_m, wq), proj(n2_o, wq)).reshape(tokens, heads, head_dim)
        kv = canonical(proj(n2_m, wkv), proj(n2_o, wkv)).reshape(tokens, kv_local, head_dim)
        q_out = rotate(q, cos_t, sin_t).astype(BF16)
        kv_out = rotate(kv, cos_kv, sin_kv).astype(BF16)

        resid = give(h2_m)
        grad_hidden = give(dh_m)
        return (resid, q_out, kv_out, grad_hidden, reduce_gain(gg_ffn), reduce_gain(gg_attn), gw_gate, gw_up, gw_down,
                gw_q.reshape(w_q.shape), gw_kv.reshape(w_kv.shape))

    row_spec = P(("dp", "ty"), "tx")
    head_spec = P(("dp", "tx"), "ty", None)
    in_specs = (row_spec, P(("dp", "tx")), P("tx"), P("tx", "ty"), P("tx", "ty"), P("ty", "tx"), P("tx"), P("tx", "ty", None), P("tx", "ty", None), row_spec, head_spec, head_spec)
    out_specs = (row_spec, head_spec, head_spec, row_spec, P(("dp", "tx")), P(("dp", "tx")), P(("dp", "tx"), "ty"), P(("dp", "tx"), "ty"), P(("dp", "ty"), "tx"), head_spec, head_spec)
    return jax.shard_map(local_step, mesh=mesh, in_specs=in_specs, out_specs=out_specs, check_vma=False)
```
